32 devices in a mesh: site: 4 (over z), py: 2 (over x), px: 2 (over y), pz: 2 (over core).
Axes of the slice: x: 2, y: 2, z: 4, core: 2. Of those that a mesh axis runs over, the one named last changes fastest.
Arguments:
- initial_heat_state: float32 [32, 128, 64, 128], P(('site', 'py'), 'px', 'pz'), parts along dimension 0, may hold values from 0.2 to 1.8
- scaled_speed_north: float32 [32, 128, 64, 128], P(('site', 'py'), 'px', 'pz'), parts along dimension 0, may hold values from -0.3 to 0.3
- scaled_speed_east: float32 [32, 128, 64, 128], P(('site', 'py'), 'px', 'pz'), parts along dimension 0, may hold values from -0.3 to 0.3
- scaled_speed_upward: float32 [32, 128, 64, 128], P(('site', 'py'), 'px', 'pz'), parts along dimension 0, may hold values from -0.3 to 0.3
Outputs:
- temperature_end: float32 [32, 128, 64, 128], P(('site', 'py'), 'px', 'pz'), parts along dimension 0
The draws below stay inside these ranges and needn't reach their ends.
There are 4 independent parts, one for each index of `site`. The reference program is written for one: setup_inputs(seed, part) draws one part's arguments, and reference() takes and returns one part's arrays. A program takes and returns all parts, laid end to end along the dimension named above; each array names one. Nothing has to cross between parts.
All inputs are finite; a program needn't handle non-finite values.
Results may differ from the reference program's by a relative error of at most 0.00002.
Values sent between devices are 32-bit elements; how exact they have to be, the bound alone decides.
No kernel may reach another device: no remote copies, remote signals or barrier semaphores. Data moves between devices by JAX's collectives and lax.ppermute only.
A program may use at most 256 MiB of HBM per device.

```python
import jax
import jax.numpy as jnp
from jax import lax

MESH_POINTS_NORTH = 8
MESH_POINTS_EAST = 128
MESH_POINTS_UP = 64
TRACER_TOTAL = 128
STEPS = 4


def block_scale(key, shape, pieces, least, largest):
    gain, own = 1.0, jax.random.fold_in(key, 6)
    for position, blocks in pieces:
        heights = jnp.exp(jax.random.uniform(jax.random.fold_in(own, position), (blocks,), jnp.float32, least / len(pieces), largest / len(pieces)))
        gain = gain * jnp.repeat(heights, shape[position] // blocks).reshape([-1 if axis == position else 1 for axis in range(len(shape))])
    return gain


def setup_inputs(seed: int = 0, part: int = 0) -> dict:
    splits = jax.random.split(jax.random.key(seed), 5)
    part_keys = jax.random.split(jax.random.fold_in(splits[4], part), 5)
    return {
        "initial_heat_state": jnp.clip(0.2 + 1.5999999 * jax.random.uniform(part_keys[0], (MESH_POINTS_NORTH, MESH_POINTS_EAST, MESH_POINTS_UP, TRACER_TOTAL), jnp.float32) ** block_scale(part_keys[0], (MESH_POINTS_NORTH, MESH_POINTS_EAST, MESH_POINTS_UP, TRACER_TOTAL), ((0, 2), (1, 2), (2, 2)), -0.2, 0.2), 0.2, 1.8),
        "scaled_speed_north": jnp.clip(jax.random.uniform(part_keys[1], (MESH_POINTS_NORTH, MESH_POINTS_EAST, MESH_POINTS_UP, TRACER_TOTAL), jnp.float32, -0.3, 0.3) * block_scale(part_keys[1], (MESH_POINTS_NORTH, MESH_POINTS_EAST, MESH_POINTS_UP, TRACER_TOTAL), ((0, 2), (1, 2), (2, 2)), -0.4, 0.0), -0.3, 0.3),
        "scaled_speed_east": jnp.clip(jax.random.uniform(part_keys[2], (MESH_POINTS_NORTH, MESH_POINTS_EAST, MESH_POINTS_UP, TRACER_TOTAL), jnp.float32, -0.3, 0.3) * block_scale(part_keys[2], (MESH_POINTS_NORTH, MESH_POINTS_EAST, MESH_POINTS_UP, TRACER_TOTAL), ((0, 2), (1, 2), (2, 2)), -0.4, 0.0), -0.3, 0.3),
        "scaled_speed_upward": jnp.clip(jax.random.uniform(part_keys[3], (MESH_POINTS_NORTH, MESH_POINTS_EAST, MESH_POINTS_UP, TRACER_TOTAL), jnp.float32, -0.3, 0.3) * block_scale(part_keys[3], (MESH_POINTS_NORTH, MESH_POINTS_EAST, MESH_POINTS_UP, TRACER_TOTAL), ((0, 2), (1, 2), (2, 2)), -0.4, 0.0), -0.3, 0.3),
    }


def strip_edges(values, dims):
    for dim in dims:
        values = lax.slice_in_dim(values, 1, values.shape[dim] - 1, axis=dim)
    return values


def neighbour(values, dim, start, dims):
    others = [other for other in dims if other != dim]
    values = strip_edges(values, others)
    return lax.slice_in_dim(values, start, start + values.shape[dim] - 2, axis=dim)


def march_once(padded_with_frame, scaled_speed_north, scaled_speed_east, scaled_speed_upward):
    middle = strip_edges(padded_with_frame, (0, 1, 2))
    lower = [neighbour(padded_with_frame, dim, 0, (0, 1, 2)) for dim in (0, 1, 2)]
    upper = [neighbour(padded_with_frame, dim, 2, (0, 1, 2)) for dim in (0, 1, 2)]
    slopes = [above - below for above, below in zip(upper, lower)]
    smooth_rate = 0.05
    spread = lower[0] + upper[0] + lower[1] + upper[1] + lower[2] + upper[2] - 6.0 * middle
    return middle - scaled_speed_north * slopes[0] - scaled_speed_east * slopes[1] - scaled_speed_upward * slopes[2] + smooth_rate * spread


def reference(initial_heat_state, scaled_speed_north, scaled_speed_east, scaled_speed_upward):
    for step in range(STEPS):
        initial_heat_state = march_once(jnp.pad(initial_heat_state, ((1, 1), (1, 1), (1, 1), (0, 0)), mode="constant"), scaled_speed_north, scaled_speed_east, scaled_speed_upward)
    return initial_heat_state
```

```python
import functools

import jax
import jax.numpy as jnp
from jax import lax
from jax.experimental import pallas as pl
from jax.experimental.pallas import tpu as pltpu
from jax.sharding import PartitionSpec as P

STEPS = 4
RATE = 0.05
CHUNKS = 2
VMEM = pltpu.VMEM


def cuts(extent):
    pieces = CHUNKS if extent % (8 * CHUNKS) == 0 else 1
    width = extent // pieces
    return [(start, width) for start in range(0, extent, width)]


def exchange(faces, axis):
    count = lax.axis_size(axis)
    if count == 1:
        return []
    if count == 2:
        return [lax.ppermute(faces[0], axis, [(0, 1), (1, 0)])]
    low, high = faces
    return [
        lax.ppermute(high, axis, [(i, i + 1) for i in range(count - 1)]),
        lax.ppermute(low, axis, [(i + 1, i) for i in range(count - 1)]),
    ]


def face_count(axis):
    return min(lax.axis_size(axis) - 1, 2)


def on_sides(axis, low, high):
    count = lax.axis_size(axis)
    if count == 1:
        return
    place = lax.axis_index(axis)
    pl.when(place > 0)(low)
    pl.when(place < count - 1)(high)


def send_sides(axis, faces, low, high):
    if len(faces) == 1:
        on_sides(axis, lambda: low(faces[0]), lambda: high(faces[0]))
    elif faces:
        low(faces[0])
        high(faces[1])


def flat(ref):
    rows = 1
    for extent in ref.shape[:-1]:
        rows *= extent
    return ref.reshape(rows, ref.shape[-1])


def copy_column_layer(parts, layer, face):
    for part, start in parts:
        ny, nx, nz, _ = part.shape
        rows = flat(part)
        for y in range(ny):
            for x in range(0, nx, 8):
                face[y, pl.ds(start + x, 8), :] = rows[pl.ds((y * nx + x) * nz + layer, 8, stride=nz), :]


def send_x_and_z(parts, x_faces, z_faces):
    first, last = parts[0][0], parts[-1][0]

    def x_layer(part, row):
        def write(face):
            face[...] = part[:, row]

        return write

    send_sides("px", x_faces, x_layer(first, 0), x_layer(last, last.shape[1] - 1))
    nz = first.shape[2]
    send_sides(
        "pz",
        z_faces,
        lambda face: copy_column_layer(parts, 0, face),
        lambda face: copy_column_layer(parts, nz - 1, face),
    )


def first_y_kernel(start, width, field, *rest):
    *faces, sem = rest

    def fetch(layer, face, slot):
        copy = pltpu.make_async_copy(field.at[layer, pl.ds(start, width)], face, sem.at[slot])
        copy.start()
        copy.wait()

    top = field.shape[0] - 1
    if len(faces) == 1:
        on_sides("py", lambda: fetch(0, faces[0], 0), lambda: fetch(top, faces[0], 0))
    else:
        fetch(0, faces[0], 0)
        fetch(top, faces[1], 1)


def first_xz_kernel(nx_faces, field, *faces):
    send_x_and_z([(field, 0)], faces[:nx_faces], faces[nx_faces:])


def step_kernel(plan, *refs):
    refs = list(refs)

    def take(count):
        taken, refs[:] = refs[:count], refs[count:]
        return taken

    start, width, extent = plan["start"], plan["width"], plan["extent"]
    parts = list(zip(take(len(plan["starts"])), plan["starts"]))
    north, east, upward = take(3)
    y_halo, x_halo, z_halo = take(plan["ny_faces"]), take(plan["nx_faces"]), take(plan["nz_faces"])
    final, last_chunk = plan["final"], start + width == extent
    if final:
        if start > 0:
            take(1)
        (whole,) = take(1)
        out, sem = take(2)
    else:
        earlier = list(zip(take(len(plan["earlier"])), plan["earlier"]))
        (out,) = take(1)
        y_faces = take(plan["ny_faces"])
        if last_chunk:
            x_faces, z_faces = take(plan["nx_faces"]), take(plan["nz_faces"])

    ny, _, nz, lanes = out.shape
    layer_of = lax.broadcasted_iota(jnp.int32, (nz, lanes), 0)

    def find(x):
        for part, origin in reversed(parts):
            if x >= origin:
                return part, x - origin

    centre_part, centre_base = find(start)

    def row(x_local, left, right):
        centre = [centre_part[y, centre_base + x_local] for y in range(ny)]
        for y in range(ny):
            here = centre[y]
            above = centre[y + 1] if y + 1 < ny else None
            below = centre[y - 1] if y > 0 else None
            up = jnp.where(layer_of == nz - 1, 0.0, pltpu.roll(here, nz - 1, 0))
            down = jnp.where(layer_of == 0, 0.0, pltpu.roll(here, 1, 0))
            total = here * (1.0 - 6.0 * RATE)
            spread = up + down
            total -= upward[y, start + x_local] * (up - down)
            for speed, higher, lower in ((north, above, below), (east, right and right(y), left and left(y))):
                if higher is None and lower is None:
                    continue
                rate = speed[y, start + x_local]
                if lower is None:
                    total -= rate * higher
                    spread += higher
                elif higher is None:
                    total += rate * lower
                    spread += lower
                else:
                    total -= rate * (higher - lower)
                    spread += higher + lower
            out[y, x_local] = total + RATE * spread

    def at(part, index):
        return lambda y: part[y, index]

    def edge(x):
        return at(*find(x)) if 0 <= x < extent else None

    row(0, edge(start - 1), edge(start + 1))

    @pl.loop(1, width - 1)
    def _(x):
        row(x, at(centre_part, centre_base + x - 1), at(centre_part, centre_base + x + 1))

    row(width - 1, edge(start + width - 2), edge(start + width))

    def y_side(layer, sign, halo):
        def add():
            @pl.loop(0, width)
            def _(x):
                out[layer, x] += (RATE + sign * north[layer, start + x]) * halo[x]

        return add

    if y_halo:
        on_sides("py", y_side(0, 1.0, y_halo[0]), y_side(ny - 1, -1.0, y_halo[-1]))

    def x_side(x, sign, halo):
        def add():
            for y in range(ny):
                out[y, x - start] += (RATE + sign * east[y, x]) * halo[y]

        return add

    if x_halo:
        nothing = lambda: None
        on_sides(
            "px",
            x_side(0, 1.0, x_halo[0]) if start == 0 else nothing,
            x_side(extent - 1, -1.0, x_halo[-1]) if last_chunk else nothing,
        )

    def z_side(layer, sign, halo):
        def add():
            out_rows, up_rows = flat(out), flat(upward)
            for y in range(ny):
                for x in range(0, width, 8):
                    mine = pl.ds((y * width + x) * nz + layer, 8, stride=nz)
                    speed = up_rows[pl.ds((y * extent + start + x) * nz + layer, 8, stride=nz), :]
                    out_rows[mine, :] = out_rows[mine, :] + (RATE + sign * speed) * halo[y, pl.ds(start + x, 8), :]

        return add

    if z_halo:
        on_sides("pz", z_side(0, 1.0, z_halo[0]), z_side(nz - 1, -1.0, z_halo[-1]))

    if final:
        copy = pltpu.make_async_copy(out, whole.at[:, pl.ds(start, width)], sem)
        copy.start()
        copy.wait()
        return

    def y_layer(layer):
        def write(face):
            face[...] = out[layer]

        return write

    send_sides("py", y_faces, y_layer(0), y_layer(ny - 1))
    if last_chunk:
        send_x_and_z(earlier + [(out, start)], x_faces, z_faces)


def body(field, north, east, upward):
    ny, nx, nz, lanes = field.shape
    counts = [face_count(axis) for axis in ("py", "px", "pz")]
    chunks = cuts(nx)
    in_vmem = pl.BlockSpec(memory_space=VMEM)
    anywhere = pl.BlockSpec(memory_space=pl.ANY)
    params = pltpu.CompilerParams(vmem_limit_bytes=8 * 2**20)

    def vmem(*shape):
        return VMEM(shape, field.dtype)

    def call(kernel, outs, ins, in_specs=None, flops=0, **more):
        more.setdefault("out_specs", [in_vmem] * len(outs))
        return list(
            pl.pallas_call(
                kernel,
                out_shape=outs,
                in_specs=in_specs or [in_vmem] * len(ins),
                compiler_params=params,
                cost_estimate=pl.CostEstimate(flops=flops, bytes_accessed=0, transcendentals=0),
                **more,
            )(*ins)
        )

    y_halos = []
    for start, width in chunks:
        faces = []
        if counts[0]:
            faces = call(
                functools.partial(first_y_kernel, start, width),
                [vmem(width, nz, lanes)] * counts[0],
                [pltpu.with_memory_space_constraint(field, pltpu.HBM)],
                [anywhere],
                flops=10**6,
                scratch_shapes=[pltpu.SemaphoreType.DMA((2,))],
            )
        y_halos.append(exchange(faces, "py"))
    x_shapes = [vmem(ny, nz, lanes)] * counts[1]
    z_shapes = [vmem(ny, nx, lanes)] * counts[2]
    faces = []
    if counts[1] + counts[2]:
        faces = call(functools.partial(first_xz_kernel, counts[1]), x_shapes + z_shapes, [field], flops=10**6)
    x_halo, z_halo = exchange(faces[: counts[1]], "px"), exchange(faces[counts[1] :], "pz")

    parts, starts = [field], [0]
    whole = None
    for step in range(STEPS):
        final = step == STEPS - 1
        new_parts, new_halos = [], []
        for index, (start, width) in enumerate(chunks):
            last_chunk = index == len(chunks) - 1
            plan = dict(
                start=start,
                width=width,
                extent=nx,
                starts=starts,
                ny_faces=counts[0],
                nx_faces=counts[1],
                nz_faces=counts[2],
                final=final,
                earlier=[begin for begin, _ in chunks[:index]] if last_chunk and not final else [],
            )
            ins = parts + [north, east, upward] + y_halos[index] + x_halo + z_halo
            flops = 20 * ny * width * nz * lanes
            if final:
                specs = [in_vmem] * len(ins)
                alias = {}
                if whole is not None:
                    alias = {len(ins): 0}
                    ins, specs = ins + [whole], specs + [anywhere]
                (whole,) = call(
                    functools.partial(step_kernel, plan),
                    [jax.ShapeDtypeStruct(field.shape, field.dtype)],
                    ins,
                    specs,
                    flops=flops,
                    out_specs=[anywhere],
                    input_output_aliases=alias,
                    scratch_shapes=[VMEM((ny, width, nz, lanes), field.dtype), pltpu.SemaphoreType.DMA],
                )
                continue
            outs = [vmem(ny, width, nz, lanes)] + [vmem(width, nz, lanes)] * counts[0]
            if last_chunk:
                outs += x_shapes + z_shapes
                ins += new_parts
            made = call(functools.partial(step_kernel, plan), outs, ins, flops=flops)
            new_parts.append(made[0])
            y_faces, rest = made[1 : 1 + counts[0]], made[1 + counts[0] :]
            new_halos.append(exchange(y_faces, "py"))
        if not final:
            x_halo, z_halo = exchange(rest[: counts[1]], "px"), exchange(rest[counts[1] :], "pz")
            parts, starts, y_halos = new_parts, [begin for begin, _ in chunks], new_halos
    return whole


def solution(mesh):
    spec = P(("site", "py"), "px", "pz", None)
    return jax.shard_map(body, mesh=mesh, in_specs=(spec,) * 4, out_specs=spec, check_vma=False)
```

```python
import functools

import jax
import jax.numpy as jnp
from jax import lax
from jax.experimental import pallas as pl
from jax.experimental.pallas import tpu as pltpu
from jax.sharding import PartitionSpec as P


STEPS = 4
RATE = 0.05
CHUNKS = 2
ROWS = 8
VMEM = pltpu.VMEM


def cuts(extent):
    pieces = CHUNKS if extent % (ROWS * CHUNKS) == 0 else 1
    width = extent // pieces
    return [(start, width) for start in range(0, extent, width)]


def split(start, width, first):
    if 0 < first < width:
        return [(start, first), (start + first, width - first)]
    return [(start, width)]


def exchange(faces, axis):
    count = lax.axis_size(axis)
    if count == 1:
        return []
    if count == 2:
        return [lax.ppermute(faces[0], axis, [(0, 1), (1, 0)])]
    low, high = faces
    return [
        lax.ppermute(high, axis, [(i, i + 1) for i in range(count - 1)]),
        lax.ppermute(low, axis, [(i + 1, i) for i in range(count - 1)]),
    ]


def face_count(axis):
    return min(lax.axis_size(axis) - 1, 2)


def on_sides(axis, low, high):
    count = lax.axis_size(axis)
    if count == 1:
        return
    place = lax.axis_index(axis)
    pl.when(place > 0)(low)
    pl.when(place < count - 1)(high)


def send_sides(axis, faces, low, high):
    if len(faces) == 1:
        on_sides(axis, lambda: low(faces[0]), lambda: high(faces[0]))
    elif faces:
        low(faces[0])
        high(faces[1])


def flat(ref):
    rows = 1
    for extent in ref.shape[:-1]:
        rows *= extent
    return ref.reshape(rows, ref.shape[-1])


def copy_column_layer(parts, layer, face):
    for part, start in parts:
        ny, nx, nz, _ = part.shape
        rows = flat(part)
        for y in range(ny):
            for x in range(0, nx, ROWS):
                face[y, pl.ds(start + x, ROWS), :] = rows[pl.ds((y * nx + x) * nz + layer, ROWS, stride=nz), :]


def send_x_and_z(parts, x_faces, z_faces):
    first, last = parts[0][0], parts[-1][0]

    def x_layer(part, row):
        def write(face):
            face[...] = part[:, row]

        return write

    send_sides("px", x_faces, x_layer(first, 0), x_layer(last, last.shape[1] - 1))
    nz = first.shape[2]
    send_sides(
        "pz",
        z_faces,
        lambda face: copy_column_layer(parts, 0, face),
        lambda face: copy_column_layer(parts, nz - 1, face),
    )


def first_y_kernel(pieces, sides, field, after, *rest):
    faces, sem = rest[: len(pieces) * sides], rest[-1]
    top = field.shape[0] - 1

    def fetch(layers):
        copies = []
        for index, (start, width) in enumerate(pieces):
            for side, layer in enumerate(layers):
                slot = index * sides + side
                copies.append(pltpu.make_async_copy(field.at[layer, pl.ds(start, width)], faces[slot], sem.at[slot]))
        for copy in copies:
            copy.start()
        for copy in copies:
            copy.wait()

    if sides == 1:
        on_sides("py", lambda: fetch([0]), lambda: fetch([top]))
    else:
        fetch([0, top])


def load_field_kernel(nx_faces, field, after, copy_of, *rest):
    faces, sem = rest[:-1], rest[-1]
    copy = pltpu.make_async_copy(field, copy_of, sem)
    copy.start()
    copy.wait()
    send_x_and_z([(copy_of, 0)], faces[:nx_faces], faces[nx_faces:])


def load_speeds_kernel(north, east, upward, after, *rest):
    *held, sem = rest
    copies = [
        pltpu.make_async_copy(speed, place, sem.at[slot])
        for slot, (speed, place) in enumerate(zip((north, east, upward), held))
    ]
    for copy in copies:
        copy.start()
    for copy in copies:
        copy.wait()


def march(out, start, width, extent, parts, speeds, x_halo, z_halo):
    north, east, upward = speeds
    ny, _, nz, lanes = out.shape
    layer_of = lax.broadcasted_iota(jnp.int32, (nz, lanes), 0)

    def find(x):
        for part, origin in reversed(parts):
            if x >= origin:
                return part, x - origin

    centre_part, centre_base = find(start)

    def row(x_local, left, right):
        centre = [centre_part[y, centre_base + x_local] for y in range(ny)]
        for y in range(ny):
            here = centre[y]
            above = centre[y + 1] if y + 1 < ny else None
            below = centre[y - 1] if y > 0 else None
            up = jnp.where(layer_of == nz - 1, 0.0, pltpu.roll(here, nz - 1, 0))
            down = jnp.where(layer_of == 0, 0.0, pltpu.roll(here, 1, 0))
            total = here * (1.0 - 6.0 * RATE)
            spread = up + down
            total -= upward[y, start + x_local] * (up - down)
            for speed, higher, lower in ((north, above, below), (east, right and right(y), left and left(y))):
                if higher is None and lower is None:
                    continue
                rate = speed[y, start + x_local]
                if lower is None:
                    total -= rate * higher
                    spread += higher
                elif higher is None:
                    total += rate * lower
                    spread += lower
                else:
                    total -= rate * (higher - lower)
                    spread += higher + lower
            out[y, x_local] = total + RATE * spread

    def at(part, index):
        return lambda y: part[y, index]

    def edge(x):
        return at(*find(x)) if 0 <= x < extent else None

    row(0, edge(start - 1), edge(start + 1))

    @pl.loop(1, width - 1)
    def _(x):
        row(x, at(centre_part, centre_base + x - 1), at(centre_part, centre_base + x + 1))

    row(width - 1, edge(start + width - 2), edge(start + width))

    def x_side(x, sign, halo):
        def add():
            for y in range(ny):
                out[y, x - start] += (RATE + sign * east[y, x]) * halo[y]

        return add

    if x_halo:
        nothing = lambda: None
        on_sides(
            "px",
            x_side(0, 1.0, x_halo[0]) if start == 0 else nothing,
            x_side(extent - 1, -1.0, x_halo[-1]) if start + width == extent else nothing,
        )

    def z_side(layer, sign, halo):
        def add():
            out_rows, up_rows = flat(out), flat(upward)
            for y in range(ny):
                for x in range(0, width, ROWS):
                    mine = pl.ds((y * width + x) * nz + layer, ROWS, stride=nz)
                    speed = up_rows[pl.ds((y * extent + start + x) * nz + layer, ROWS, stride=nz), :]
                    out_rows[mine, :] = out_rows[mine, :] + (RATE + sign * speed) * halo[y, pl.ds(start + x, ROWS), :]

        return add

    if z_halo:
        on_sides("pz", z_side(0, 1.0, z_halo[0]), z_side(nz - 1, -1.0, z_halo[-1]))


def taker(refs):
    refs = list(refs)

    def take(count):
        taken, refs[:] = refs[:count], refs[count:]
        return taken

    return take


def step_kernel(plan, *refs):
    take = taker(refs)
    start, width, extent, sides = plan["start"], plan["width"], plan["extent"], plan["sides"]
    parts = list(zip(take(len(plan["starts"])), plan["starts"]))
    speeds = take(3)
    x_halo, z_halo = take(sides[1]), take(sides[2])
    y_halos = [(piece, take(sides[0])) for piece in plan["arrive"]]
    earlier = list(zip(take(len(plan["earlier"])), plan["earlier"]))
    (out,) = take(1)
    y_faces = [(piece, take(sides[0])) for piece in plan["leave"]]
    north, ny = speeds[0], out.shape[0]

    march(out, start, width, extent, parts, speeds, x_halo, z_halo)

    def y_side(layer, sign, side):
        def add():
            for (begin, count), halo in y_halos:

                @pl.loop(0, count)
                def _(x):
                    out[layer, begin - start + x] += (RATE + sign * north[layer, begin + x]) * halo[side][x]

        return add

    if sides[0]:
        on_sides("py", y_side(0, 1.0, 0), y_side(ny - 1, -1.0, sides[0] - 1))

    def y_layer(layer, begin, count):
        def write(face):
            face[...] = out[layer, pl.ds(begin - start, count)]

        return write

    for (begin, count), faces in y_faces:
        send_sides("py", faces, y_layer(0, begin, count), y_layer(ny - 1, begin, count))
    if start + width == extent:
        x_faces, z_faces = take(sides[1]), take(sides[2])
        send_x_and_z(earlier + [(out, start)], x_faces, z_faces)


def last_inner_kernel(plan, *refs):
    take = taker(refs)
    extent, sides = plan["extent"], plan["sides"]
    parts = list(zip(take(len(plan["starts"])), plan["starts"]))
    speeds = take(3)
    x_halo, z_halo = take(sides[1]), take(sides[2])
    (whole,) = take(1)
    waiting = take(sides[0])
    outs = take(len(plan["chunks"]))
    (sem,) = take(1)
    ny = whole.shape[0]

    def ready(index, begin, count):
        start, width = plan["chunks"][index]
        return pltpu.make_async_copy(
            outs[index].at[pl.ds(begin, count)], whole.at[pl.ds(begin, count), pl.ds(start, width)], sem.at[index]
        )

    def put(index, start, width):
        def keep(layer):
            def write(face):
                face[pl.ds(start, width)] = outs[index][layer]

            return write

        send_sides("py", waiting, keep(0), keep(ny - 1))
        if sides[0] == 0:
            ready(index, 0, ny).start()
        elif sides[0] == 1:
            on_sides("py", ready(index, 1, ny - 1).start, ready(index, 0, ny - 1).start)
        elif ny > 2:
            ready(index, 1, ny - 2).start()

    for index, (start, width) in enumerate(plan["chunks"]):
        march(outs[index], start, width, extent, parts, speeds, x_halo, z_halo)
        put(index, start, width)
    for index in range(len(plan["chunks"])):
        count = ny - sides[0]
        if count > 0:
            ready(index, 0, count).wait()


def last_outer_kernel(piece, sides, north, *refs):
    take = taker(refs)
    waiting, halo = take(sides), take(sides)
    take(1)
    (whole,) = take(1)
    held = take(sides)
    (sem,) = take(1)
    begin, count = piece
    top = whole.shape[0] - 1

    def finish(layer, sign, side):
        def run():
            for x in range(count):
                rate = RATE + sign * north[layer, begin + x]
                held[side][x] = waiting[side][begin + x] + rate * halo[side][x]
            copy = pltpu.make_async_copy(held[side], whole.at[layer, pl.ds(begin, count)], sem.at[side])
            copy.start()
            copy.wait()

        return run

    low, high = finish(0, 1.0, 0), finish(top, -1.0, sides - 1)
    if sides == 1:
        on_sides("py", low, high)
    else:
        low()
        high()


def body(field, north, east, upward):
    ny, nx, nz, lanes = field.shape
    sides = [face_count(axis) for axis in ("py", "px", "pz")]
    chunks = cuts(nx)
    in_vmem = pl.BlockSpec(memory_space=VMEM)
    anywhere = pl.BlockSpec(memory_space=pl.ANY)
    dma = pltpu.SemaphoreType.DMA
    params = pltpu.CompilerParams(vmem_limit_bytes=12 * 2**20)

    def vmem(*shape):
        return VMEM(shape, field.dtype)

    def call(kernel, outs, ins, in_specs=None, flops=0, **more):
        more.setdefault("out_specs", [in_vmem] * len(outs))
        return list(
            pl.pallas_call(
                kernel,
                out_shape=outs,
                in_specs=in_specs or [in_vmem] * len(ins),
                compiler_params=params,
                cost_estimate=pl.CostEstimate(flops=flops, bytes_accessed=0, transcendentals=0),
                **more,
            )(*ins)
        )

    def in_hbm(array):
        return pltpu.with_memory_space_constraint(array, pltpu.HBM)

    def send_y(pieces, faces):
        halos = []
        for i in range(len(pieces)):
            halos.append(exchange(faces[i * sides[0] : (i + 1) * sides[0]], "py"))
        return halos

    arrive = [split(*chunk, ROWS if index == 0 else 0) for index, chunk in enumerate(chunks)]
    pieces = [piece for chunk in arrive for piece in chunk]
    halos, after = [], in_hbm(north)
    for group in (pieces[:1], pieces[1:]):
        if sides[0] and group:
            faces = call(
                functools.partial(first_y_kernel, group, sides[0]),
                [vmem(width, nz, lanes) for _, width in group for _ in range(sides[0])],
                [in_hbm(field), after],
                [anywhere] * 2,
                flops=10**6,
                scratch_shapes=[dma((len(group) * sides[0],))],
            )
            after = faces[0]
            halos += send_y(group, faces)
        else:
            halos += [[] for _ in group]
    x_shapes = [vmem(ny, nz, lanes)] * sides[1]
    z_shapes = [vmem(ny, nx, lanes)] * sides[2]
    field, *faces = call(
        functools.partial(load_field_kernel, sides[1]),
        [vmem(*field.shape)] + x_shapes + z_shapes,
        [in_hbm(field), after],
        [anywhere] * 2,
        flops=10**6,
        scratch_shapes=[dma],
    )
    x_halo, z_halo = exchange(faces[: sides[1]], "px"), exchange(faces[sides[1] :], "pz")
    speeds = call(
        load_speeds_kernel,
        [vmem(*field.shape)] * 3,
        [in_hbm(speed) for speed in (north, east, upward)] + [field],
        [anywhere] * 4,
        flops=10**7,
        scratch_shapes=[dma((3,))],
    )

    parts, starts = [field], [0]
    for step in range(STEPS - 1):
        new_parts, new_halos, new_arrive = [], [], []
        for index, chunk in enumerate(chunks):
            start, width = chunk
            last_chunk = index == len(chunks) - 1
            tail = step == STEPS - 2 and last_chunk
            leave = split(start, width, width - ROWS if tail else 0)
            plan = dict(
                start=start,
                width=width,
                extent=nx,
                starts=starts,
                sides=sides,
                arrive=arrive[index],
                leave=leave,
                earlier=[begin for begin, _ in chunks[:index]] if last_chunk else [],
            )
            mine, halos = halos[: len(arrive[index])], halos[len(arrive[index]) :]
            ins = parts + speeds + x_halo + z_halo + [half for piece in mine for half in piece]
            outs = [vmem(ny, width, nz, lanes)] + [vmem(count, nz, lanes) for _, count in leave for _ in range(sides[0])]
            if last_chunk:
                outs += x_shapes + z_shapes
                ins += new_parts
            made = call(functools.partial(step_kernel, plan), outs, ins, flops=20 * ny * width * nz * lanes)
            new_parts.append(made[0])
            faces, rest = made[1 : 1 + sides[0] * len(leave)], made[1 + sides[0] * len(leave) :]
            new_halos += send_y(leave, faces)
            new_arrive.append(leave)
        x_halo, z_halo = exchange(rest[: sides[1]], "px"), exchange(rest[sides[1] :], "pz")
        parts, starts, halos, arrive = new_parts, [begin for begin, _ in chunks], new_halos, new_arrive

    whole, *waiting = call(
        functools.partial(last_inner_kernel, dict(extent=nx, starts=starts, sides=sides, chunks=chunks)),
        [jax.ShapeDtypeStruct(parts[0].shape[:1] + (nx, nz, lanes), north.dtype)] + [vmem(nx, nz, lanes)] * sides[0],
        parts + speeds + x_halo + z_halo,
        flops=20 * ny * nx * nz * lanes,
        out_specs=[anywhere] + [in_vmem] * sides[0],
        scratch_shapes=[vmem(ny, width, nz, lanes) for _, width in chunks] + [dma((len(chunks),))],
    )
    if sides[0]:
        pieces = [piece for chunk in arrive for piece in chunk]
        for piece, halo in zip(pieces, halos):
            ins = speeds[:1] + waiting + halo + [whole]
            (whole,) = call(
                functools.partial(last_outer_kernel, piece, sides[0]),
                [jax.ShapeDtypeStruct(whole.shape, whole.dtype)],
                ins,
                [in_vmem] * (len(ins) - 1) + [anywhere],
                flops=3 * piece[1] * nz * lanes,
                out_specs=[anywhere],
                input_output_aliases={len(ins) - 1: 0},
                scratch_shapes=[vmem(piece[1], nz, lanes)] * sides[0] + [dma((sides[0],))],
            )
    return whole


def solution(mesh):
    spec = P(("site", "py"), "px", "pz", None)

    return jax.shard_map(body, mesh=mesh, in_specs=(spec,) * 4, out_specs=spec, check_vma=False)
```

```python
import functools

import jax
import jax.numpy as jnp
from jax import lax
from jax.experimental import pallas as pl
from jax.experimental.pallas import tpu as pltpu
from jax.sharding import PartitionSpec as P


STEPS = 4
RATE = 0.05
CHUNKS = 2
ROWS = 8
FIRST = 16
VMEM = pltpu.VMEM


def cuts(extent):
    pieces = CHUNKS if extent % (ROWS * CHUNKS) == 0 else 1
    width = extent // pieces
    return [(start, width) for start in range(0, extent, width)]


def split(start, width, first):
    if 0 < first < width:
        return [(start, first), (start + first, width - first)]
    return [(start, width)]


def exchange(faces, axis):
    count = lax.axis_size(axis)
    if count == 1:
        return []
    if count == 2:
        return [lax.ppermute(faces[0], axis, [(0, 1), (1, 0)])]
    low, high = faces
    return [
        lax.ppermute(high, axis, [(i, i + 1) for i in range(count - 1)]),
        lax.ppermute(low, axis, [(i + 1, i) for i in range(count - 1)]),
    ]


def face_count(axis):
    return min(lax.axis_size(axis) - 1, 2)


def on_sides(axis, low, high):
    count = lax.axis_size(axis)
    if count == 1:
        return
    place = lax.axis_index(axis)
    pl.when(place > 0)(low)
    pl.when(place < count - 1)(high)


def send_sides(axis, faces, low, high):
    if len(faces) == 1:
        on_sides(axis, lambda: low(faces[0]), lambda: high(faces[0]))
    elif faces:
        low(faces[0])
        high(faces[1])


def flat(ref):
    rows = 1
    for extent in ref.shape[:-1]:
        rows *= extent
    return ref.reshape(rows, ref.shape[-1])


def copy_column_layer(parts, layer, face):
    for part, start in parts:
        ny, nx, nz, _ = part.shape
        rows = flat(part)
        for y in range(ny):
            for x in range(0, nx, ROWS):
                face[y, pl.ds(start + x, ROWS), :] = rows[pl.ds((y * nx + x) * nz + layer, ROWS, stride=nz), :]


def send_x_and_z(parts, x_faces, z_faces):
    first, last = parts[0][0], parts[-1][0]

    def x_layer(part, row):
        def write(face):
            face[...] = part[:, row]

        return write

    send_sides("px", x_faces, x_layer(first, 0), x_layer(last, last.shape[1] - 1))
    nz = first.shape[2]
    send_sides(
        "pz",
        z_faces,
        lambda face: copy_column_layer(parts, 0, face),
        lambda face: copy_column_layer(parts, nz - 1, face),
    )


def load(sources, places, sem, slot, priority=0):
    copies = [
        pltpu.make_async_copy(source, place, sem.at[slot + i]) for i, (source, place) in enumerate(zip(sources, places))
    ]
    for copy in copies:
        copy.start(priority=priority)
    for copy in copies:
        copy.wait()


def first_y_kernel(pieces, sides, field, after, *rest):
    *rest, sem = rest
    speeds, rest = (rest[:3], rest[3:]) if len(rest) > len(pieces) * sides else ([], rest)
    faces, held = rest[: len(pieces) * sides], rest[len(pieces) * sides :]
    if speeds:
        pl.when(lax.axis_index("pz") % 2 == 1)(lambda: load(speeds, held, sem, len(faces)))
    top = field.shape[0] - 1

    def fetch(layers):
        sources = [field.at[layer, pl.ds(start, width)] for start, width in pieces for layer in layers]
        load(sources, faces, sem, 0, 1 - len(speeds) // 3)

    if sides == 1:
        fetch([top * (1 - lax.axis_index("py"))])
    else:
        fetch([0, top])


def load_field_kernel(nx_faces, field, after, copy_of, *rest):
    faces, sem = rest[:-1], rest[-1]
    copy = pltpu.make_async_copy(field, copy_of, sem)
    copy.start()
    copy.wait()
    send_x_and_z([(copy_of, 0)], faces[:nx_faces], faces[nx_faces:])


def load_speeds_kernel(partly, north, east, upward, after, *rest):
    *held, sem = rest[3 * partly :]
    fetch = lambda: load((north, east, upward), held, sem, 0)
    if partly:
        pl.when(lax.axis_index("pz") % 2 == 0)(fetch)
    else:
        fetch()


def march(out, start, width, extent, parts, speeds, x_halo, z_halo):
    north, east, upward = speeds
    ny, _, nz, lanes = out.shape
    layer_of = lax.broadcasted_iota(jnp.int32, (nz, lanes), 0)

    def find(x):
        for part, origin in reversed(parts):
            if x >= origin:
                return part, x - origin

    centre_part, centre_base = find(start)

    def row(x_local, left, right):
        centre = [centre_part[y, centre_base + x_local] for y in range(ny)]
        for y in range(ny):
            here = centre[y]
            above = centre[y + 1] if y + 1 < ny else None
            below = centre[y - 1] if y > 0 else None
            up = jnp.where(layer_of == nz - 1, 0.0, pltpu.roll(here, nz - 1, 0))
            down = jnp.where(layer_of == 0, 0.0, pltpu.roll(here, 1, 0))
            total = here * (1.0 - 6.0 * RATE)
            spread = up + down
            total -= upward[y, start + x_local] * (up - down)
            for speed, higher, lower in ((north, above, below), (east, right and right(y), left and left(y))):
                if higher is None and lower is None:
                    continue
                rate = speed[y, start + x_local]
                if lower is None:
                    total -= rate * higher
                    spread += higher
                elif higher is None:
                    total += rate * lower
                    spread += lower
                else:
                    total -= rate * (higher - lower)
                    spread += higher + lower
            out[y, x_local] = total + RATE * spread

    def at(part, index):
        return lambda y: part[y, index]

    def edge(x):
        return at(*find(x)) if 0 <= x < extent else None

    row(0, edge(start - 1), edge(start + 1))

    @pl.loop(1, width - 1)
    def _(x):
        row(x, at(centre_part, centre_base + x - 1), at(centre_part, centre_base + x + 1))

    row(width - 1, edge(start + width - 2), edge(start + width))

    def x_side(x, sign, halo):
        def add():
            for y in range(ny):
                out[y, x - start] += (RATE + sign * east[y, x]) * halo[y]

        return add

    if x_halo:
        nothing = lambda: None
        on_sides(
            "px",
            x_side(0, 1.0, x_halo[0]) if start == 0 else nothing,
            x_side(extent - 1, -1.0, x_halo[-1]) if start + width == extent else nothing,
        )

    def z_side(layer, sign, halo):
        def add():
            out_rows, up_rows = flat(out), flat(upward)
            for y in range(ny):
                for x in range(0, width, ROWS):
                    mine = pl.ds((y * width + x) * nz + layer, ROWS, stride=nz)
                    speed = up_rows[pl.ds((y * extent + start + x) * nz + layer, ROWS, stride=nz), :]
                    out_rows[mine, :] = out_rows[mine, :] + (RATE + sign * speed) * halo[y, pl.ds(start + x, ROWS), :]

        return add

    if z_halo:
        on_sides("pz", z_side(0, 1.0, z_halo[0]), z_side(nz - 1, -1.0, z_halo[-1]))


def taker(refs):
    refs = list(refs)

    def take(count):
        taken, refs[:] = refs[:count], refs[count:]
        return taken

    return take


def step_kernel(plan, *refs):
    take = taker(refs)
    start, width, extent, sides = plan["start"], plan["width"], plan["extent"], plan["sides"]
    parts = list(zip(take(len(plan["starts"])), plan["starts"]))
    speeds = take(3)
    x_halo, z_halo = take(sides[1]), take(sides[2])
    y_halos = [(piece, take(sides[0])) for piece in plan["arrive"]]
    earlier = list(zip(take(len(plan["earlier"])), plan["earlier"]))
    (out,) = take(1)
    y_faces = [(piece, take(sides[0])) for piece in plan["leave"]]
    north, ny = speeds[0], out.shape[0]

    march(out, start, width, extent, parts, speeds, x_halo, z_halo)

    def y_side(layer, sign, side):
        def add():
            for (begin, count), halo in y_halos:

                @pl.loop(0, count)
                def _(x):
                    out[layer, begin - start + x] += (RATE + sign * north[layer, begin + x]) * halo[side][x]

        return add

    if sides[0]:
        on_sides("py", y_side(0, 1.0, 0), y_side(ny - 1, -1.0, sides[0] - 1))

    def y_layer(layer, begin, count):
        def write(face):
            face[...] = out[layer, pl.ds(begin - start, count)]

        return write

    for (begin, count), faces in y_faces:
        send_sides("py", faces, y_layer(0, begin, count), y_layer(ny - 1, begin, count))
    if start + width == extent:
        x_faces, z_faces = take(sides[1]), take(sides[2])
        send_x_and_z(earlier + [(out, start)], x_faces, z_faces)


def last_inner_kernel(plan, *refs):
    take = taker(refs)
    extent, sides = plan["extent"], plan["sides"]
    parts = list(zip(take(len(plan["starts"])), plan["starts"]))
    speeds = take(3)
    x_halo, z_halo = take(sides[1]), take(sides[2])
    (whole,) = take(1)
    waiting = take(sides[0])
    outs = take(len(plan["chunks"]))
    (sem,) = take(1)
    ny = whole.shape[0]

    def ready(index, begin, count):
        start, width = plan["chunks"][index]
        return pltpu.make_async_copy(
            outs[index].at[pl.ds(begin, count)], whole.at[pl.ds(begin, count), pl.ds(start, width)], sem.at[index]
        )

    def put(index, start, width):
        def keep(layer):
            def write(face):
                face[pl.ds(start, width)] = outs[index][layer]

            return write

        send_sides("py", waiting, keep(0), keep(ny - 1))
        if sides[0] == 0:
            ready(index, 0, ny).start()
        elif sides[0] == 1:
            on_sides("py", ready(index, 1, ny - 1).start, ready(index, 0, ny - 1).start)
        elif ny > 2:
            ready(index, 1, ny - 2).start()

    for index, (start, width) in enumerate(plan["chunks"]):
        march(outs[index], start, width, extent, parts, speeds, x_halo, z_halo)
        put(index, start, width)
    for index in range(len(plan["chunks"])):
        count = ny - sides[0]
        if count > 0:
            ready(index, 0, count).wait()


def last_outer_kernel(piece, sides, north, *refs):
    take = taker(refs)
    waiting, halo = take(sides), take(sides)
    take(1)
    (whole,) = take(1)
    held = take(sides)
    (sem,) = take(1)
    begin, count = piece
    top = whole.shape[0] - 1

    def finish(layer, sign, side):
        def run():
            for x in range(count):
                rate = RATE + sign * north[layer, begin + x]
                held[side][x] = waiting[side][begin + x] + rate * halo[side][x]
            copy = pltpu.make_async_copy(held[side], whole.at[layer, pl.ds(begin, count)], sem.at[side])
            copy.start(priority=1)
            copy.wait()

        return run

    low, high = finish(0, 1.0, 0), finish(top, -1.0, sides - 1)
    if sides == 1:
        on_sides("py", low, high)
    else:
        low()
        high()


def body(field, north, east, upward):
    ny, nx, nz, lanes = field.shape
    sides = [face_count(axis) for axis in ("py", "px", "pz")]
    chunks = cuts(nx)
    in_vmem = pl.BlockSpec(memory_space=VMEM)
    anywhere = pl.BlockSpec(memory_space=pl.ANY)
    dma = pltpu.SemaphoreType.DMA
    params = pltpu.CompilerParams(vmem_limit_bytes=12 * 2**20)

    def vmem(*shape):
        return VMEM(shape, field.dtype)

    def call(kernel, outs, ins, in_specs=None, flops=0, **more):
        more.setdefault("out_specs", [in_vmem] * len(outs))
        return list(
            pl.pallas_call(
                kernel,
                out_shape=outs,
                in_specs=in_specs or [in_vmem] * len(ins),
                compiler_params=params,
                cost_estimate=pl.CostEstimate(flops=flops, bytes_accessed=0, transcendentals=0),
                **more,
            )(*ins)
        )

    def in_hbm(array):
        return pltpu.with_memory_space_constraint(array, pltpu.HBM)

    def send_y(pieces, faces):
        halos = []
        for i in range(len(pieces)):
            halos.append(exchange(faces[i * sides[0] : (i + 1) * sides[0]], "py"))
        return halos

    arrive = [split(*chunk, FIRST if index == 0 else 0) for index, chunk in enumerate(chunks)]
    pieces = [piece for chunk in arrive for piece in chunk]
    speeds = [in_hbm(speed) for speed in (north, east, upward)]
    halos, held, after = [], [], speeds[0]
    for group, early in ((pieces[:1], []), (pieces[1:], speeds)):
        if sides[0] == 0:
            halos += [[] for _ in group]
        elif group:
            shapes = [vmem(width, nz, lanes) for _, width in group for _ in range(sides[0])]
            made = call(
                functools.partial(first_y_kernel, group, sides[0]),
                shapes + [vmem(*field.shape)] * len(early),
                [in_hbm(field), after] + early,
                [anywhere] * (2 + len(early)),
                flops=10**6,
                scratch_shapes=[dma((len(shapes) + len(early),))],
            )
            faces, held = made[: len(shapes)], made[len(shapes) :]
            after = faces[0]
            halos += send_y(group, faces)
    x_shapes = [vmem(ny, nz, lanes)] * sides[1]
    z_shapes = [vmem(ny, nx, lanes)] * sides[2]
    field, *faces = call(
        functools.partial(load_field_kernel, sides[1]),
        [vmem(*field.shape)] + x_shapes + z_shapes,
        [in_hbm(field), after],
        [anywhere] * 2,
        flops=10**6,
        scratch_shapes=[dma],
    )
    x_halo, z_halo = exchange(faces[: sides[1]], "px"), exchange(faces[sides[1] :], "pz")
    speeds = call(
        functools.partial(load_speeds_kernel, len(held) > 0),
        [vmem(*field.shape)] * 3,
        speeds + [field] + held,
        [anywhere] * (4 + len(held)),
        flops=10**7,
        out_specs=[anywhere] * 3,
        input_output_aliases={4 + i: i for i in range(len(held))},
        scratch_shapes=[dma((3,))],
    )

    parts, starts = [field], [0]
    for step in range(STEPS - 1):
        new_parts, new_halos, new_arrive = [], [], []
        for index, chunk in enumerate(chunks):
            start, width = chunk
            last_chunk = index == len(chunks) - 1
            tail = step == STEPS - 2 and last_chunk
            leave = split(start, width, width - ROWS if tail else 0)
            plan = dict(
                start=start,
                width=width,
                extent=nx,
                starts=starts,
                sides=sides,
                arrive=arrive[index],
                leave=leave,
                earlier=[begin for begin, _ in chunks[:index]] if last_chunk else [],
            )
            mine, halos = halos[: len(arrive[index])], halos[len(arrive[index]) :]
            ins = parts + speeds + x_halo + z_halo + [half for piece in mine for half in piece]
            outs = [vmem(ny, width, nz, lanes)] + [vmem(count, nz, lanes) for _, count in leave for _ in range(sides[0])]
            if last_chunk:
                outs += x_shapes + z_shapes
                ins += new_parts
            made = call(functools.partial(step_kernel, plan), outs, ins, flops=20 * ny * width * nz * lanes)
            new_parts.append(made[0])
            faces, rest = made[1 : 1 + sides[0] * len(leave)], made[1 + sides[0] * len(leave) :]
            new_halos += send_y(leave, faces)
            new_arrive.append(leave)
        x_halo, z_halo = exchange(rest[: sides[1]], "px"), exchange(rest[sides[1] :], "pz")
        parts, starts, halos, arrive = new_parts, [begin for begin, _ in chunks], new_halos, new_arrive

    whole, *waiting = call(
        functools.partial(last_inner_kernel, dict(extent=nx, starts=starts, sides=sides, chunks=chunks)),
        [jax.ShapeDtypeStruct(parts[0].shape[:1] + (nx, nz, lanes), north.dtype)] + [vmem(nx, nz, lanes)] * sides[0],
        parts + speeds + x_halo + z_halo,
        flops=20 * ny * nx * nz * lanes,
        out_specs=[anywhere] + [in_vmem] * sides[0],
        scratch_shapes=[vmem(ny, width, nz, lanes) for _, width in chunks] + [dma((len(chunks),))],
    )
    if sides[0]:
        pieces = [piece for chunk in arrive for piece in chunk]
        for piece, halo in zip(pieces, halos):
            ins = speeds[:1] + waiting + halo + [whole]
            (whole,) = call(
                functools.partial(last_outer_kernel, piece, sides[0]),
                [jax.ShapeDtypeStruct(whole.shape, whole.dtype)],
                ins,
                [in_vmem] * (len(ins) - 1) + [anywhere],
                flops=3 * piece[1] * nz * lanes,
                out_specs=[anywhere],
                input_output_aliases={len(ins) - 1: 0},
                scratch_shapes=[vmem(piece[1], nz, lanes)] * sides[0] + [dma((sides[0],))],
            )
    return whole


def solution(mesh):
    spec = P(("site", "py"), "px", "pz", None)

    return jax.shard_map(body, mesh=mesh, in_specs=(spec,) * 4, out_specs=spec, check_vma=False)
```

```python
import functools

import jax
import jax.numpy as jnp
from jax import lax
from jax.experimental import pallas as pl
from jax.experimental.pallas import tpu as pltpu
from jax.sharding import PartitionSpec as P


STEPS = 4
RATE = 0.05
CHUNKS = 2
ROWS = 8
FIRST = 16
VMEM = pltpu.VMEM


def cuts(extent):
    pieces = CHUNKS if extent % (ROWS * CHUNKS) == 0 else 1
    width = extent // pieces
    return [(start, width) for start in range(0, extent, width)]


def split(start, width, first):
    if 0 < first < width:
        return [(start, first), (start + first, width - first)]
    return [(start, width)]


def exchange(faces, axis):
    count = lax.axis_size(axis)
    if count == 1:
        return []
    if count == 2:
        return [lax.ppermute(faces[0], axis, [(0, 1), (1, 0)])]
    low, high = faces
    return [
        lax.ppermute(high, axis, [(i, i + 1) for i in range(count - 1)]),
        lax.ppermute(low, axis, [(i + 1, i) for i in range(count - 1)]),
    ]


def face_count(axis):
    return min(lax.axis_size(axis) - 1, 2)


def on_sides(axis, low, high):
    count = lax.axis_size(axis)
    if count == 1:
        return
    place = lax.axis_index(axis)
    pl.when(place > 0)(low)
    pl.when(place < count - 1)(high)


def send_sides(axis, faces, low, high):
    if len(faces) == 1:
        on_sides(axis, lambda: low(faces[0]), lambda: high(faces[0]))
    elif faces:
        low(faces[0])
        high(faces[1])


def flat(ref):
    rows = 1
    for extent in ref.shape[:-1]:
        rows *= extent
    return ref.reshape(rows, ref.shape[-1])


def copy_column_layer(parts, layer, face):
    for part, start in parts:
        ny, nx, nz, _ = part.shape
        rows = flat(part)
        for y in range(ny):
            for x in range(0, nx, ROWS):
                face[y, pl.ds(start + x, ROWS), :] = rows[pl.ds((y * nx + x) * nz + layer, ROWS, stride=nz), :]


def send_x_and_z(parts, x_faces, z_faces):
    first, last = parts[0][0], parts[-1][0]

    def x_layer(part, row):
        def write(face):
            face[...] = part[:, row]

        return write

    send_sides("px", x_faces, x_layer(first, 0), x_layer(last, last.shape[1] - 1))
    nz = first.shape[2]
    send_sides(
        "pz",
        z_faces,
        lambda face: copy_column_layer(parts, 0, face),
        lambda face: copy_column_layer(parts, nz - 1, face),
    )


def load(sources, places, sem, slot):
    copies = [
        pltpu.make_async_copy(source, place, sem.at[slot + i]) for i, (source, place) in enumerate(zip(sources, places))
    ]
    for copy in copies:
        copy.start()
    for copy in copies:
        copy.wait()


def first_y_kernel(pieces, sides, field, after, *rest):
    *rest, sem = rest
    speeds, rest = (rest[:3], rest[3:]) if len(rest) > len(pieces) * sides else ([], rest)
    faces, held = rest[: len(pieces) * sides], rest[len(pieces) * sides :]
    if speeds:
        pl.when(lax.axis_index("pz") % 2 == 1)(lambda: load(speeds, held, sem, len(faces)))
    top = field.shape[0] - 1

    def fetch(layers):
        sources = [field.at[layer, pl.ds(start, width)] for start, width in pieces for layer in layers]
        load(sources, faces, sem, 0)

    if sides == 1:
        on_sides("py", lambda: fetch([0]), lambda: fetch([top]))
    else:
        fetch([0, top])


def load_field_kernel(nx_faces, field, after, copy_of, *rest):
    faces, sem = rest[:-1], rest[-1]
    copy = pltpu.make_async_copy(field, copy_of, sem)
    copy.start()
    copy.wait()
    send_x_and_z([(copy_of, 0)], faces[:nx_faces], faces[nx_faces:])


def load_speeds_kernel(partly, north, east, upward, after, *rest):
    *held, sem = rest[3 * partly :]
    fetch = lambda: load((north, east, upward), held, sem, 0)
    if partly:
        pl.when(lax.axis_index("pz") % 2 == 0)(fetch)
    else:
        fetch()


def march(out, start, width, extent, parts, speeds, x_halo, z_halo):
    north, east, upward = speeds
    ny, _, nz, lanes = out.shape
    layer_of = lax.broadcasted_iota(jnp.int32, (nz, lanes), 0)

    def find(x):
        for part, origin in reversed(parts):
            if x >= origin:
                return part, x - origin

    centre_part, centre_base = find(start)

    def row(x_local, left, right):
        centre = [centre_part[y, centre_base + x_local] for y in range(ny)]
        for y in range(ny):
            here = centre[y]
            above = centre[y + 1] if y + 1 < ny else None
            below = centre[y - 1] if y > 0 else None
            up = jnp.where(layer_of == nz - 1, 0.0, pltpu.roll(here, nz - 1, 0))
            down = jnp.where(layer_of == 0, 0.0, pltpu.roll(here, 1, 0))
            total = here * (1.0 - 6.0 * RATE)
            spread = up + down
            total -= upward[y, start + x_local] * (up - down)
            for speed, higher, lower in ((north, above, below), (east, right and right(y), left and left(y))):
                if higher is None and lower is None:
                    continue
                rate = speed[y, start + x_local]
                if lower is None:
                    total -= rate * higher
                    spread += higher
                elif higher is None:
                    total += rate * lower
                    spread += lower
                else:
                    total -= rate * (higher - lower)
                    spread += higher + lower
            out[y, x_local] = total + RATE * spread

    def at(part, index):
        return lambda y: part[y, index]

    def edge(x):
        return at(*find(x)) if 0 <= x < extent else None

    row(0, edge(start - 1), edge(start + 1))

    @pl.loop(1, width - 1)
    def _(x):
        row(x, at(centre_part, centre_base + x - 1), at(centre_part, centre_base + x + 1))

    row(width - 1, edge(start + width - 2), edge(start + width))

    def x_side(x, sign, halo):
        def add():
            for y in range(ny):
                out[y, x - start] += (RATE + sign * east[y, x]) * halo[y]

        return add

    if x_halo:
        nothing = lambda: None
        on_sides(
            "px",
            x_side(0, 1.0, x_halo[0]) if start == 0 else nothing,
            x_side(extent - 1, -1.0, x_halo[-1]) if start + width == extent else nothing,
        )

    def z_side(layer, sign, halo):
        def add():
            out_rows, up_rows = flat(out), flat(upward)
            for y in range(ny):
                for x in range(0, width, ROWS):
                    mine = pl.ds((y * width + x) * nz + layer, ROWS, stride=nz)
                    speed = up_rows[pl.ds((y * extent + start + x) * nz + layer, ROWS, stride=nz), :]
                    out_rows[mine, :] = out_rows[mine, :] + (RATE + sign * speed) * halo[y, pl.ds(start + x, ROWS), :]

        return add

    if z_halo:
        on_sides("pz", z_side(0, 1.0, z_halo[0]), z_side(nz - 1, -1.0, z_halo[-1]))


def taker(refs):
    refs = list(refs)

    def take(count):
        taken, refs[:] = refs[:count], refs[count:]
        return taken

    return take


def step_kernel(plan, *refs):
    take = taker(refs)
    start, width, extent, sides = plan["start"], plan["width"], plan["extent"], plan["sides"]
    parts = list(zip(take(len(plan["starts"])), plan["starts"]))
    speeds = take(3)
    x_halo, z_halo = take(sides[1]), take(sides[2])
    y_halos = [(piece, take(sides[0])) for piece in plan["arrive"]]
    earlier = list(zip(take(len(plan["earlier"])), plan["earlier"]))
    (out,) = take(1)
    y_faces = [(piece, take(sides[0])) for piece in plan["leave"]]
    north, ny = speeds[0], out.shape[0]

    march(out, start, width, extent, parts, speeds, x_halo, z_halo)

    def y_side(layer, sign, side):
        def add():
            for (begin, count), halo in y_halos:

                @pl.loop(0, count)
                def _(x):
                    out[layer, begin - start + x] += (RATE + sign * north[layer, begin + x]) * halo[side][x]

        return add

    if sides[0]:
        on_sides("py", y_side(0, 1.0, 0), y_side(ny - 1, -1.0, sides[0] - 1))

    def y_layer(layer, begin, count):
        def write(face):
            face[...] = out[layer, pl.ds(begin - start, count)]

        return write

    for (begin, count), faces in y_faces:
        send_sides("py", faces, y_layer(0, begin, count), y_layer(ny - 1, begin, count))
    if start + width == extent:
        x_faces, z_faces = take(sides[1]), take(sides[2])
        send_x_and_z(earlier + [(out, start)], x_faces, z_faces)


def last_inner_kernel(plan, *refs):
    take = taker(refs)
    extent, sides = plan["extent"], plan["sides"]
    parts = list(zip(take(len(plan["starts"])), plan["starts"]))
    speeds = take(3)
    x_halo, z_halo = take(sides[1]), take(sides[2])
    (whole,) = take(1)
    waiting = take(sides[0])
    outs = take(len(plan["chunks"]))
    (sem,) = take(1)
    ny = whole.shape[0]

    def ready(index, begin, count):
        start, width = plan["chunks"][index]
        return pltpu.make_async_copy(
            outs[index].at[pl.ds(begin, count)], whole.at[pl.ds(begin, count), pl.ds(start, width)], sem.at[index]
        )

    def put(index, start, width):
        def keep(layer):
            def write(face):
                face[pl.ds(start, width)] = outs[index][layer]

            return write

        send_sides("py", waiting, keep(0), keep(ny - 1))
        if sides[0] == 0:
            ready(index, 0, ny).start()
        elif sides[0] == 1:
            on_sides("py", ready(index, 1, ny - 1).start, ready(index, 0, ny - 1).start)
        elif ny > 2:
            ready(index, 1, ny - 2).start()

    for index, (start, width) in enumerate(plan["chunks"]):
        march(outs[index], start, width, extent, parts, speeds, x_halo, z_halo)
        put(index, start, width)
    for index in range(len(plan["chunks"])):
        count = ny - sides[0]
        if count > 0:
            ready(index, 0, count).wait()


def last_outer_kernel(piece, sides, north, *refs):
    take = taker(refs)
    waiting, halo = take(sides), take(sides)
    take(1)
    (whole,) = take(1)
    held = take(sides)
    (sem,) = take(1)
    begin, count = piece
    top = whole.shape[0] - 1

    halves = split(0, count, count // 2)

    def finish(layer, sign, side):
        copies = []
        for slot, (first, rows) in enumerate(halves):
            for x in range(first, first + rows):
                rate = RATE + sign * north[layer, begin + x]
                held[side][x] = waiting[side][begin + x] + rate * halo[side][x]
            copies.append(
                pltpu.make_async_copy(
                    held[side].at[pl.ds(first, rows)],
                    whole.at[layer, pl.ds(begin + first, rows)],
                    sem.at[side * len(halves) + slot],
                )
            )
            copies[-1].start()
        for copy in copies:
            copy.wait()

    if sides == 1:
        place = lax.axis_index("py")
        finish(top * (1 - place), (2 * place - 1).astype(jnp.float32), 0)
    else:
        finish(0, 1.0, 0)
        finish(top, -1.0, 1)


def body(field, north, east, upward):
    ny, nx, nz, lanes = field.shape
    sides = [face_count(axis) for axis in ("py", "px", "pz")]
    chunks = cuts(nx)
    in_vmem = pl.BlockSpec(memory_space=VMEM)
    anywhere = pl.BlockSpec(memory_space=pl.ANY)
    dma = pltpu.SemaphoreType.DMA
    params = pltpu.CompilerParams(vmem_limit_bytes=12 * 2**20)

    def vmem(*shape):
        return VMEM(shape, field.dtype)

    def call(kernel, outs, ins, in_specs=None, flops=0, **more):
        more.setdefault("out_specs", [in_vmem] * len(outs))
        return list(
            pl.pallas_call(
                kernel,
                out_shape=outs,
                in_specs=in_specs or [in_vmem] * len(ins),
                compiler_params=params,
                cost_estimate=pl.CostEstimate(flops=flops, bytes_accessed=0, transcendentals=0),
                **more,
            )(*ins)
        )

    def in_hbm(array):
        return pltpu.with_memory_space_constraint(array, pltpu.HBM)

    def send_y(pieces, faces):
        halos = []
        for i in range(len(pieces)):
            halos.append(exchange(faces[i * sides[0] : (i + 1) * sides[0]], "py"))
        return halos

    arrive = [split(*chunk, FIRST if index == 0 else 0) for index, chunk in enumerate(chunks)]
    pieces = [piece for chunk in arrive for piece in chunk]
    speeds = [in_hbm(speed) for speed in (north, east, upward)]
    halos, held, after = [], [], speeds[0]
    for group, early in ((pieces[:1], []), (pieces[1:], speeds)):
        if sides[0] == 0:
            halos += [[] for _ in group]
        elif group:
            shapes = [vmem(width, nz, lanes) for _, width in group for _ in range(sides[0])]
            made = call(
                functools.partial(first_y_kernel, group, sides[0]),
                shapes + [vmem(*field.shape)] * len(early),
                [in_hbm(field), after] + early,
                [anywhere] * (2 + len(early)),
                flops=10**6,
                scratch_shapes=[dma((len(shapes) + len(early),))],
            )
            faces, held = made[: len(shapes)], made[len(shapes) :]
            after = faces[0]
            halos += send_y(group, faces)
    x_shapes = [vmem(ny, nz, lanes)] * sides[1]
    z_shapes = [vmem(ny, nx, lanes)] * sides[2]
    field, *faces = call(
        functools.partial(load_field_kernel, sides[1]),
        [vmem(*field.shape)] + x_shapes + z_shapes,
        [in_hbm(field), after],
        [anywhere] * 2,
        flops=10**6,
        scratch_shapes=[dma],
    )
    x_halo, z_halo = exchange(faces[: sides[1]], "px"), exchange(faces[sides[1] :], "pz")
    speeds = call(
        functools.partial(load_speeds_kernel, len(held) > 0),
        [vmem(*field.shape)] * 3,
        speeds + [field] + held,
        [anywhere] * (4 + len(held)),
        flops=10**7,
        out_specs=[anywhere] * 3,
        input_output_aliases={4 + i: i for i in range(len(held))},
        scratch_shapes=[dma((3,))],
    )

    parts, starts = [field], [0]
    for step in range(STEPS - 1):
        new_parts, new_halos, new_arrive = [], [], []
        for index, chunk in enumerate(chunks):
            start, width = chunk
            last_chunk = index == len(chunks) - 1
            tail = step == STEPS - 2 and last_chunk
            leave = split(start, width, width - ROWS if tail else 0)
            plan = dict(
                start=start,
                width=width,
                extent=nx,
                starts=starts,
                sides=sides,
                arrive=arrive[index],
                leave=leave,
                earlier=[begin for begin, _ in chunks[:index]] if last_chunk else [],
            )
            mine, halos = halos[: len(arrive[index])], halos[len(arrive[index]) :]
            ins = parts + speeds + x_halo + z_halo + [half for piece in mine for half in piece]
            outs = [vmem(ny, width, nz, lanes)] + [vmem(count, nz, lanes) for _, count in leave for _ in range(sides[0])]
            if last_chunk:
                outs += x_shapes + z_shapes
                ins += new_parts
            made = call(functools.partial(step_kernel, plan), outs, ins, flops=20 * ny * width * nz * lanes)
            new_parts.append(made[0])
            faces, rest = made[1 : 1 + sides[0] * len(leave)], made[1 + sides[0] * len(leave) :]
            new_halos += send_y(leave, faces)
            new_arrive.append(leave)
        x_halo, z_halo = exchange(rest[: sides[1]], "px"), exchange(rest[sides[1] :], "pz")
        parts, starts, halos, arrive = new_parts, [begin for begin, _ in chunks], new_halos, new_arrive

    whole, *waiting = call(
        functools.partial(last_inner_kernel, dict(extent=nx, starts=starts, sides=sides, chunks=chunks)),
        [jax.ShapeDtypeStruct(parts[0].shape[:1] + (nx, nz, lanes), north.dtype)] + [vmem(nx, nz, lanes)] * sides[0],
        parts + speeds + x_halo + z_halo,
        flops=20 * ny * nx * nz * lanes,
        out_specs=[anywhere] + [in_vmem] * sides[0],
        scratch_shapes=[vmem(ny, width, nz, lanes) for _, width in chunks] + [dma((len(chunks),))],
    )
    if sides[0]:
        pieces = [piece for chunk in arrive for piece in chunk]
        for piece, halo in zip(pieces, halos):
            ins = speeds[:1] + waiting + halo + [whole]
            (whole,) = call(
                functools.partial(last_outer_kernel, piece, sides[0]),
                [jax.ShapeDtypeStruct(whole.shape, whole.dtype)],
                ins,
                [in_vmem] * (len(ins) - 1) + [anywhere],
                flops=3 * piece[1] * nz * lanes,
                out_specs=[anywhere],
                input_output_aliases={len(ins) - 1: 0},
                scratch_shapes=[vmem(piece[1], nz, lanes)] * sides[0] + [dma((2 * sides[0],))],
            )
    return whole


def solution(mesh):
    spec = P(("site", "py"), "px", "pz", None)

    return jax.shard_map(body, mesh=mesh, in_specs=(spec,) * 4, out_specs=spec, check_vma=False)
```

```python
import functools

import jax
import jax.numpy as jnp
from jax import lax
from jax.experimental import pallas as pl
from jax.experimental.pallas import tpu as pltpu
from jax.sharding import PartitionSpec as P


STEPS = 4
RATE = 0.05
CHUNKS = 2
ROWS = 8
FIRST = 12
VMEM = pltpu.VMEM


def cuts(extent):
    pieces = CHUNKS if extent % (ROWS * CHUNKS) == 0 else 1
    width = extent // pieces
    return [(start, width) for start in range(0, extent, width)]


def split(start, width, first):
    if 0 < first < width:
        return [(start, first), (start + first, width - first)]
    return [(start, width)]


def exchange(faces, axis):
    count = lax.axis_size(axis)
    if count == 1:
        return []
    if count == 2:
        return [lax.ppermute(faces[0], axis, [(0, 1), (1, 0)])]
    low, high = faces
    return [
        lax.ppermute(high, axis, [(i, i + 1) for i in range(count - 1)]),
        lax.ppermute(low, axis, [(i + 1, i) for i in range(count - 1)]),
    ]


def face_count(axis):
    return min(lax.axis_size(axis) - 1, 2)


def on_sides(axis, low, high):
    count = lax.axis_size(axis)
    if count == 1:
        return
    place = lax.axis_index(axis)
    pl.when(place > 0)(low)
    pl.when(place < count - 1)(high)


def send_sides(axis, faces, low, high):
    if len(faces) == 1:
        on_sides(axis, lambda: low(faces[0]), lambda: high(faces[0]))
    elif faces:
        low(faces[0])
        high(faces[1])


def flat(ref):
    rows = 1
    for extent in ref.shape[:-1]:
        rows *= extent
    return ref.reshape(rows, ref.shape[-1])


def copy_column_layer(parts, layer, face):
    for part, start in parts:
        ny, nx, nz, _ = part.shape
        rows = flat(part)
        for y in range(ny):
            for x in range(0, nx, ROWS):
                face[y, pl.ds(start + x, ROWS), :] = rows[pl.ds((y * nx + x) * nz + layer, ROWS, stride=nz), :]


def send_x_and_z(parts, x_faces, z_faces):
    first, last = parts[0][0], parts[-1][0]

    def x_layer(part, row):
        def write(face):
            face[...] = part[:, row]

        return write

    send_sides("px", x_faces, x_layer(first, 0), x_layer(last, last.shape[1] - 1))
    nz = first.shape[2]
    send_sides(
        "pz",
        z_faces,
        lambda face: copy_column_layer(parts, 0, face),
        lambda face: copy_column_layer(parts, nz - 1, face),
    )


def load(sources, places, sem, slot):
    copies = [
        pltpu.make_async_copy(source, place, sem.at[slot + i]) for i, (source, place) in enumerate(zip(sources, places))
    ]
    for copy in copies:
        copy.start()
    for copy in copies:
        copy.wait()


def first_y_kernel(pieces, sides, field, after, *rest):
    *rest, sem = rest
    speeds, rest = (rest[:3], rest[3:]) if len(rest) > len(pieces) * sides else ([], rest)
    faces, held = rest[: len(pieces) * sides], rest[len(pieces) * sides :]
    if speeds:
        pl.when(lax.axis_index("pz") % 2 == 1)(lambda: load(speeds, held, sem, len(faces)))
    top = field.shape[0] - 1

    def fetch(layers):
        sources = [field.at[layer, pl.ds(start, width)] for start, width in pieces for layer in layers]
        load(sources, faces, sem, 0)

    if sides == 1:
        on_sides("py", lambda: fetch([0]), lambda: fetch([top]))
    else:
        fetch([0, top])


def load_field_kernel(nx_faces, field, after, copy_of, *rest):
    faces, sem = rest[:-1], rest[-1]
    copy = pltpu.make_async_copy(field, copy_of, sem)
    copy.start()
    copy.wait()
    send_x_and_z([(copy_of, 0)], faces[:nx_faces], faces[nx_faces:])


def load_speeds_kernel(partly, north, east, upward, after, *rest):
    *held, sem = rest[3 * partly :]
    fetch = lambda: load((north, east, upward), held, sem, 0)
    if partly:
        pl.when(lax.axis_index("pz") % 2 == 0)(fetch)
    else:
        fetch()


def march(out, start, width, extent, parts, speeds, x_halo, z_halo):
    north, east, upward = speeds
    ny, _, nz, lanes = out.shape
    layer_of = lax.broadcasted_iota(jnp.int32, (nz, lanes), 0)

    def find(x):
        for part, origin in reversed(parts):
            if x >= origin:
                return part, x - origin

    centre_part, centre_base = find(start)

    def row(x_local, left, right):
        centre = [centre_part[y, centre_base + x_local] for y in range(ny)]
        for y in range(ny):
            here = centre[y]
            above = centre[y + 1] if y + 1 < ny else None
            below = centre[y - 1] if y > 0 else None
            up = jnp.where(layer_of == nz - 1, 0.0, pltpu.roll(here, nz - 1, 0))
            down = jnp.where(layer_of == 0, 0.0, pltpu.roll(here, 1, 0))
            total = here * (1.0 - 6.0 * RATE)
            spread = up + down
            total -= upward[y, start + x_local] * (up - down)
            for speed, higher, lower in ((north, above, below), (east, right and right(y), left and left(y))):
                if higher is None and lower is None:
                    continue
                rate = speed[y, start + x_local]
                if lower is None:
                    total -= rate * higher
                    spread += higher
                elif higher is None:
                    total += rate * lower
                    spread += lower
                else:
                    total -= rate * (higher - lower)
                    spread += higher + lower
            out[y, x_local] = total + RATE * spread

    def at(part, index):
        return lambda y: part[y, index]

    def edge(x):
        return at(*find(x)) if 0 <= x < extent else None

    row(0, edge(start - 1), edge(start + 1))

    @pl.loop(1, width - 1)
    def _(x):
        row(x, at(centre_part, centre_base + x - 1), at(centre_part, centre_base + x + 1))

    row(width - 1, edge(start + width - 2), edge(start + width))

    def x_side(x, sign, halo):
        def add():
            for y in range(ny):
                out[y, x - start] += (RATE + sign * east[y, x]) * halo[y]

        return add

    if x_halo:
        nothing = lambda: None
        on_sides(
            "px",
            x_side(0, 1.0, x_halo[0]) if start == 0 else nothing,
            x_side(extent - 1, -1.0, x_halo[-1]) if start + width == extent else nothing,
        )

    def z_side(layer, sign, halo):
        def add():
            out_rows, up_rows = flat(out), flat(upward)
            for y in range(ny):
                for x in range(0, width, ROWS):
                    mine = pl.ds((y * width + x) * nz + layer, ROWS, stride=nz)
                    speed = up_rows[pl.ds((y * extent + start + x) * nz + layer, ROWS, stride=nz), :]
                    out_rows[mine, :] = out_rows[mine, :] + (RATE + sign * speed) * halo[y, pl.ds(start + x, ROWS), :]

        return add

    if z_halo:
        on_sides("pz", z_side(0, 1.0, z_halo[0]), z_side(nz - 1, -1.0, z_halo[-1]))


def taker(refs):
    refs = list(refs)

    def take(count):
        taken, refs[:] = refs[:count], refs[count:]
        return taken

    return take


def step_kernel(plan, *refs):
    take = taker(refs)
    start, width, extent, sides = plan["start"], plan["width"], plan["extent"], plan["sides"]
    parts = list(zip(take(len(plan["starts"])), plan["starts"]))
    speeds = take(3)
    x_halo, z_halo = take(sides[1]), take(sides[2])
    y_halos = [(piece, take(sides[0])) for piece in plan["arrive"]]
    earlier = list(zip(take(len(plan["earlier"])), plan["earlier"]))
    (out,) = take(1)
    y_faces = [(piece, take(sides[0])) for piece in plan["leave"]]
    north, ny = speeds[0], out.shape[0]

    march(out, start, width, extent, parts, speeds, x_halo, z_halo)

    def y_side(layer, sign, side):
        def add():
            for (begin, count), halo in y_halos:

                @pl.loop(0, count)
                def _(x):
                    out[layer, begin - start + x] += (RATE + sign * north[layer, begin + x]) * halo[side][x]

        return add

    if sides[0]:
        on_sides("py", y_side(0, 1.0, 0), y_side(ny - 1, -1.0, sides[0] - 1))

    def y_layer(layer, begin, count):
        def write(face):
            face[...] = out[layer, pl.ds(begin - start, count)]

        return write

    for (begin, count), faces in y_faces:
        send_sides("py", faces, y_layer(0, begin, count), y_layer(ny - 1, begin, count))
    if start + width == extent:
        x_faces, z_faces = take(sides[1]), take(sides[2])
        send_x_and_z(earlier + [(out, start)], x_faces, z_faces)


def last_inner_kernel(plan, *refs):
    take = taker(refs)
    extent, sides = plan["extent"], plan["sides"]
    parts = list(zip(take(len(plan["starts"])), plan["starts"]))
    speeds = take(3)
    x_halo, z_halo = take(sides[1]), take(sides[2])
    (whole,) = take(1)
    waiting = take(sides[0])
    outs = take(len(plan["chunks"]))
    (sem,) = take(1)
    ny = whole.shape[0]

    def ready(index, begin, count):
        start, width = plan["chunks"][index]
        return pltpu.make_async_copy(
            outs[index].at[pl.ds(begin, count)], whole.at[pl.ds(begin, count), pl.ds(start, width)], sem.at[index]
        )

    def put(index, start, width):
        def keep(layer):
            def write(face):
                face[pl.ds(start, width)] = outs[index][layer]

            return write

        send_sides("py", waiting, keep(0), keep(ny - 1))
        if sides[0] == 0:
            ready(index, 0, ny).start()
        elif sides[0] == 1:
            on_sides("py", ready(index, 1, ny - 1).start, ready(index, 0, ny - 1).start)
        elif ny > 2:
            ready(index, 1, ny - 2).start()

    for index, (start, width) in enumerate(plan["chunks"]):
        march(outs[index], start, width, extent, parts, speeds, x_halo, z_halo)
        put(index, start, width)
    for index in range(len(plan["chunks"])):
        count = ny - sides[0]
        if count > 0:
            ready(index, 0, count).wait()


def last_outer_kernel(piece, sides, north, *refs):
    take = taker(refs)
    waiting, halo = take(sides), take(sides)
    take(1)
    (whole,) = take(1)
    held = take(sides)
    (sem,) = take(1)
    begin, count = piece
    top = whole.shape[0] - 1

    def finish(layer, sign, side):
        def run():
            for x in range(count):
                rate = RATE + sign * north[layer, begin + x]
                held[side][x] = waiting[side][begin + x] + rate * halo[side][x]
            copy = pltpu.make_async_copy(held[side], whole.at[layer, pl.ds(begin, count)], sem.at[side])
            copy.start()
            copy.wait()

        return run

    low, high = finish(0, 1.0, 0), finish(top, -1.0, sides - 1)
    if sides == 1:
        on_sides("py", low, high)
    else:
        low()
        high()


def body(field, north, east, upward):
    ny, nx, nz, lanes = field.shape
    sides = [face_count(axis) for axis in ("py", "px", "pz")]
    chunks = cuts(nx)
    in_vmem = pl.BlockSpec(memory_space=VMEM)
    anywhere = pl.BlockSpec(memory_space=pl.ANY)
    dma = pltpu.SemaphoreType.DMA
    params = pltpu.CompilerParams(vmem_limit_bytes=12 * 2**20)

    def vmem(*shape):
        return VMEM(shape, field.dtype)

    def call(kernel, outs, ins, in_specs=None, flops=0, **more):
        more.setdefault("out_specs", [in_vmem] * len(outs))
        return list(
            pl.pallas_call(
                kernel,
                out_shape=outs,
                in_specs=in_specs or [in_vmem] * len(ins),
                compiler_params=params,
                cost_estimate=pl.CostEstimate(flops=flops, bytes_accessed=0, transcendentals=0),
                **more,
            )(*ins)
        )

    def in_hbm(array):
        return pltpu.with_memory_space_constraint(array, pltpu.HBM)

    def send_y(pieces, faces):
        halos = []
        for i in range(len(pieces)):
            halos.append(exchange(faces[i * sides[0] : (i + 1) * sides[0]], "py"))
        return halos

    arrive = [split(*chunk, FIRST if index == 0 else 0) for index, chunk in enumerate(chunks)]
    pieces = [piece for chunk in arrive for piece in chunk]
    speeds = [in_hbm(speed) for speed in (north, east, upward)]
    halos, held, after = [], [], speeds[0]
    for group, early in ((pieces[:1], []), (pieces[1:], speeds)):
        if sides[0] == 0:
            halos += [[] for _ in group]
        elif group:
            shapes = [vmem(width, nz, lanes) for _, width in group for _ in range(sides[0])]
            made = call(
                functools.partial(first_y_kernel, group, sides[0]),
                shapes + [vmem(*field.shape)] * len(early),
                [in_hbm(field), after] + early,
                [anywhere] * (2 + len(early)),
                flops=10**6,
                scratch_shapes=[dma((len(shapes) + len(early),))],
            )
            faces, held = made[: len(shapes)], made[len(shapes) :]
            after = faces[0]
            halos += send_y(group, faces)
    x_shapes = [vmem(ny, nz, lanes)] * sides[1]
    z_shapes = [vmem(ny, nx, lanes)] * sides[2]
    field, *faces = call(
        functools.partial(load_field_kernel, sides[1]),
        [vmem(*field.shape)] + x_shapes + z_shapes,
        [in_hbm(field), after],
        [anywhere] * 2,
        flops=10**6,
        scratch_shapes=[dma],
    )
    x_halo, z_halo = exchange(faces[: sides[1]], "px"), exchange(faces[sides[1] :], "pz")
    speeds = call(
        functools.partial(load_speeds_kernel, len(held) > 0),
        [vmem(*field.shape)] * 3,
        speeds + [field] + held,
        [anywhere] * (4 + len(held)),
        flops=10**7,
        out_specs=[anywhere] * 3,
        input_output_aliases={4 + i: i for i in range(len(held))},
        scratch_shapes=[dma((3,))],
    )

    parts, starts = [field], [0]
    for step in range(STEPS - 1):
        new_parts, new_halos, new_arrive = [], [], []
        for index, chunk in enumerate(chunks):
            start, width = chunk
            last_chunk = index == len(chunks) - 1
            tail = step == STEPS - 2 and last_chunk
            leave = split(start, width, width - ROWS if tail else 0)
            plan = dict(
                start=start,
                width=width,
                extent=nx,
                starts=starts,
                sides=sides,
                arrive=arrive[index],
                leave=leave,
                earlier=[begin for begin, _ in chunks[:index]] if last_chunk else [],
            )
            mine, halos = halos[: len(arrive[index])], halos[len(arrive[index]) :]
            ins = parts + speeds + x_halo + z_halo + [half for piece in mine for half in piece]
            outs = [vmem(ny, width, nz, lanes)] + [vmem(count, nz, lanes) for _, count in leave for _ in range(sides[0])]
            if last_chunk:
                outs += x_shapes + z_shapes
                ins += new_parts
            made = call(functools.partial(step_kernel, plan), outs, ins, flops=20 * ny * width * nz * lanes)
            new_parts.append(made[0])
            faces, rest = made[1 : 1 + sides[0] * len(leave)], made[1 + sides[0] * len(leave) :]
            new_halos += send_y(leave, faces)
            new_arrive.append(leave)
        x_halo, z_halo = exchange(rest[: sides[1]], "px"), exchange(rest[sides[1] :], "pz")
        parts, starts, halos, arrive = new_parts, [begin for begin, _ in chunks], new_halos, new_arrive

    whole, *waiting = call(
        functools.partial(last_inner_kernel, dict(extent=nx, starts=starts, sides=sides, chunks=chunks)),
        [jax.ShapeDtypeStruct(parts[0].shape[:1] + (nx, nz, lanes), north.dtype)] + [vmem(nx, nz, lanes)] * sides[0],
        parts + speeds + x_halo + z_halo,
        flops=20 * ny * nx * nz * lanes,
        out_specs=[anywhere] + [in_vmem] * sides[0],
        scratch_shapes=[vmem(ny, width, nz, lanes) for _, width in chunks] + [dma((len(chunks),))],
    )
    if sides[0]:
        pieces = [piece for chunk in arrive for piece in chunk]
        for piece, halo in zip(pieces, halos):
            ins = speeds[:1] + waiting + halo + [whole]
            (whole,) = call(
                functools.partial(last_outer_kernel, piece, sides[0]),
                [jax.ShapeDtypeStruct(whole.shape, whole.dtype)],
                ins,
                [in_vmem] * (len(ins) - 1) + [anywhere],
                flops=3 * piece[1] * nz * lanes,
                out_specs=[anywhere],
                input_output_aliases={len(ins) - 1: 0},
                scratch_shapes=[vmem(piece[1], nz, lanes)] * sides[0] + [dma((sides[0],))],
            )
    return whole


def solution(mesh):
    spec = P(("site", "py"), "px", "pz", None)

    return jax.shard_map(body, mesh=mesh, in_specs=(spec,) * 4, out_specs=spec, check_vma=False)
```
